32 devices in a mesh: leaf: 8 (over y, x, core), front: 4 (over z).
Axes of the slice: x: 2, y: 2, z: 4, core: 2. Of those that a mesh axis runs over, the one named last changes fastest.
Arguments:
- leaf_pivot_block: bfloat16 [8, 2048, 256], P('leaf', 'front'), may hold values from -6 to 6
- leaf_rest_block: bfloat16 [8, 512, 256], P('leaf', 'front'), may hold values from -6 to 6
- node_pivot_block: bfloat16 [8, 2048, 256], P('leaf', 'front'), may hold values from -6 to 6
- node_rest_block: bfloat16 [8, 512, 256], P('leaf', 'front'), may hold values from -6 to 6
- leaf_vectors_pivot: bfloat16 [8, 2, 2048, 2048], P('leaf', None, 'front'), may hold values from -0.125 to 0.125
- leaf_vectors_rest: bfloat16 [8, 2, 512, 2048], P('leaf', None, 'front'), may hold values from -0.125 to 0.125
- node_vectors_pivot: bfloat16 [8, 2, 2048, 2048], P('leaf', None, 'front'), may hold values from -0.125 to 0.125
- node_vectors_rest: bfloat16 [8, 2, 512, 2048], P('leaf', None, 'front'), may hold values from -0.125 to 0.125
- stack_place: int32 [8, 1024], P('leaf'), may hold values from 0 to 2559, as said below
- parent_columns: int32 [8, 2, 512], P('leaf'), may hold values from 0 to 2047, as said below
- coupling: bfloat16 [8, 2, 2048, 512], P('leaf', None, 'front'), may hold values from -0.125 to 0.125
- pivot_inverse: bfloat16 [8, 2, 2048, 2048], P('leaf', None, 'front'), may hold values from -0.125 to 0.125
Outputs:
- solution: bfloat16 [8, 2, 2048, 256], P('leaf', None, 'front')
- remainder: bfloat16 [8, 512, 256], P('leaf', 'front')
The draws below stay inside these ranges and needn't reach their ends.
Inputs may be any that keep to these rules, and one draw needn't show every extreme that they name: `stack_place`: each group's row holds 1024 distinct stack rows. `parent_columns`: each group's row for each slot holds 512 distinct pivot columns.
All inputs are finite; a program needn't handle non-finite values.
Results may differ from the reference program's by a relative error of at most 0.024.
Values may be sent and summed in bfloat16 or wider, within the bound.
A program may use at most 64 MiB of HBM per device.

```python
import jax
import jax.numpy as jnp
from jax import lax

K = 2048
C = 512
R = 256
LEVELS = 2
M = 2560
GROUPS = 8
N_FRONT = 4


def draw_stack_place(key, part):
    subkeys = jax.random.split(jax.random.fold_in(key, 17), GROUPS)

    def pick_rows(subkey):
        return jax.random.permutation(subkey, K + C)[:2 * C]
    return jax.vmap(pick_rows)(subkeys).astype(jnp.int32)


def draw_parent_columns(key, part):
    subkeys = jax.random.split(jax.random.fold_in(key, 29), GROUPS * 2)

    def pick_columns(subkey):
        return jax.random.permutation(subkey, K)[:C]
    picked = jax.vmap(pick_columns)(subkeys)
    return picked.reshape(GROUPS, 2, C).astype(jnp.int32)


def shard_levels(own_key, shape, cuts, low, top_value):
    factor_of, own = 1.0, jax.random.fold_in(own_key, 6)
    for dim, parts in cuts:
        heights = jnp.exp(jax.random.uniform(jax.random.fold_in(own, dim), (parts,), jnp.float32, low / len(cuts), top_value / len(cuts)))
        factor_of = factor_of * jnp.repeat(heights, shape[dim] // parts).reshape([-1 if axis == dim else 1 for axis in range(len(shape))])
    return factor_of


def scatter_about(own_key, extent, scale, bound, cuts=(), held_as=jnp.bfloat16):
    gain = shard_levels(own_key, extent, cuts, -0.22, 0.18) if cuts else 1.0
    values = jax.random.normal(own_key, extent, jnp.float32) * scale * gain
    return jnp.minimum(jnp.maximum(values, -bound), bound).astype(held_as)


def setup_inputs(seed: int = 0) -> dict:
    streams_of = jax.random.split(jax.random.key(seed), 13)
    return {
        "leaf_pivot_block": scatter_about(streams_of[0], (GROUPS, K, R), 1.0, 6.0, ((0, 8), (1, 4))),
        "leaf_rest_block": scatter_about(streams_of[1], (GROUPS, C, R), 1.0, 6.0, ((0, 8), (1, 4))),
        "node_pivot_block": scatter_about(streams_of[2], (GROUPS, K, R), 1.0, 6.0, ((0, 8), (1, 4))),
        "node_rest_block": scatter_about(streams_of[3], (GROUPS, C, R), 1.0, 6.0, ((0, 8), (1, 4))),
        "leaf_vectors_pivot": scatter_about(streams_of[4], (GROUPS, 2, K, K), M ** -0.5, 0.125, ((0, 8), (2, 4))),
        "leaf_vectors_rest": scatter_about(streams_of[5], (GROUPS, 2, C, K), M ** -0.5, 0.125, ((0, 8), (2, 4))),
        "node_vectors_pivot": scatter_about(streams_of[6], (GROUPS, 2, K, K), M ** -0.5, 0.125, ((0, 8), (2, 4))),
        "node_vectors_rest": scatter_about(streams_of[7], (GROUPS, 2, C, K), M ** -0.5, 0.125, ((0, 8), (2, 4))),
        "stack_place": draw_stack_place(jax.random.fold_in(streams_of[12], 71), 0),
        "parent_columns": draw_parent_columns(jax.random.fold_in(streams_of[12], 71), 0),
        "coupling": scatter_about(streams_of[10], (GROUPS, 2, K, C), (4 * C) ** -0.5, 0.125, ((0, 8), (2, 4))),
        "pivot_inverse": scatter_about(streams_of[11], (GROUPS, 2, K, K), K ** -0.5, 0.125, ((0, 8), (2, 4))),
    }


def reflect(block_pivot, block_rest, vectors_pivot, vectors_rest):
    blocks = N_FRONT

    def partials(vectors, values):
        count = vectors.shape[1]
        left_side = vectors[1].reshape(blocks, count // blocks, K).astype(jnp.float32)
        right_side = values.reshape(blocks, count // blocks, R).astype(jnp.float32)
        return jnp.einsum("bik,bir->bkr", left_side, right_side)

    partial_value = partials(vectors_pivot, block_pivot) + partials(vectors_rest, block_rest)
    rounded = lax.optimization_barrier(partial_value.astype(jnp.bfloat16)).astype(jnp.float32)
    summed = jnp.sum(rounded, axis=0).astype(jnp.bfloat16)
    pivots = block_pivot.astype(jnp.float32) - jnp.dot(vectors_pivot[0], summed, preferred_element_type=jnp.float32)
    rest = block_rest.astype(jnp.float32) - jnp.dot(vectors_rest[0], summed, preferred_element_type=jnp.float32)
    return pivots.astype(jnp.bfloat16), rest.astype(jnp.bfloat16)


def reflect_all(block_pivot, block_rest, vectors_pivot, vectors_rest):
    def one_group(items):
        return reflect(items[0], items[1], items[2], items[3])

    return lax.map(one_group, (block_pivot, block_rest, vectors_pivot, vectors_rest))


def shifted(values, amount):
    if amount == 0:
        return values
    return jnp.roll(values, amount, axis=0)


def added(first, second):
    return (first.astype(jnp.float32) + second.astype(jnp.float32)).astype(jnp.bfloat16)


def reference(leaf_pivot_block, leaf_rest_block, node_pivot_block, node_rest_block, leaf_vectors_pivot, leaf_vectors_rest, node_vectors_pivot, node_vectors_rest, stack_place, parent_columns, coupling, pivot_inverse):
    subtree = 2 ** LEVELS
    leaf_pivots, leaf_remainder = reflect_all(leaf_pivot_block, leaf_rest_block, leaf_vectors_pivot, leaf_vectors_rest)

    def run_nodes(left_part, right_part):
        def place(own_pivot, own_rest, rows, left_one, right_one):
            joined = jnp.concatenate([left_one, right_one], axis=0)
            stack = jnp.concatenate([own_pivot, own_rest], axis=0)
            stack = stack.at[rows].set(joined)
            return stack[:K], stack[K:]

        stack_pivots, stack_rest = jax.vmap(place)(node_pivot_block, node_rest_block, stack_place, left_part, right_part)
        return reflect_all(stack_pivots, stack_rest, node_vectors_pivot, node_vectors_rest)

    node_pivots, node_remainder = run_nodes(shifted(leaf_remainder, 1), leaf_remainder)
    for height in range(2, LEVELS + 1):
        offset = 2 ** (height - 2)
        node_pivots, node_remainder = run_nodes(shifted(node_remainder, offset), shifted(node_remainder, -offset))
    root_part = shifted(node_remainder, -(subtree // 2))
    node_pivots, node_remainder = run_nodes(root_part, jnp.zeros_like(root_part))

    def settle_all(pivots, which_slot, parent):
        def one_group(own, columns, couple, inverse, parent_one):
            right_side = own.astype(jnp.float32)
            if parent_one is not None:
                chosen = parent_one[columns]
                right_side = right_side - jnp.dot(couple, chosen, preferred_element_type=jnp.float32)
            result = jnp.dot(inverse, right_side.astype(jnp.bfloat16), preferred_element_type=jnp.float32)
            return result.astype(jnp.bfloat16)

        if parent is None:
            return jax.vmap(lambda own, inverse: one_group(own, None, None, inverse, None))(pivots, pivot_inverse[:, which_slot])
        return jax.vmap(one_group)(pivots, parent_columns[:, which_slot], coupling[:, which_slot], pivot_inverse[:, which_slot], parent)

    node_solution = settle_all(node_pivots, 1, None)
    for height in range(LEVELS, 0, -1):
        if height == LEVELS:
            parent_part = shifted(node_solution, subtree // 2)
        else:
            offset = 2 ** (height - 1)
            parent_part = added(shifted(node_solution, -offset), shifted(node_solution, offset))
        node_solution = settle_all(node_pivots, 1, parent_part)
    parent_part = added(shifted(node_solution, -1), node_solution)
    leaf_solution = settle_all(leaf_pivots, 0, parent_part)
    solution = jnp.stack([leaf_solution, node_solution], axis=1)
    return solution, node_remainder
```

```python
import jax
import jax.numpy as jnp
from jax import lax
from jax.sharding import PartitionSpec as P

LEVELS = 2


def from_behind(block, axis, distance):
    devices = range(lax.axis_size(axis))
    route = [((i - distance) % len(devices), i) for i in devices]
    return lax.ppermute(block, axis, route)


def added(first, second):
    return (first.astype(jnp.float32) + second.astype(jnp.float32)).astype(jnp.bfloat16)


def per_device(
    leaf_pivot_block,
    leaf_rest_block,
    node_pivot_block,
    node_rest_block,
    leaf_vectors_pivot,
    leaf_vectors_rest,
    node_vectors_pivot,
    node_vectors_rest,
    stack_place,
    parent_columns,
    coupling,
    pivot_inverse,
):
    subtree = 2**LEVELS
    front_index = lax.axis_index("front")
    pivot_count = leaf_vectors_pivot.shape[2]
    rest_count = leaf_vectors_rest.shape[2]
    depth = leaf_vectors_pivot.shape[3]
    rest_rows_all = stack_place.shape[1] // 2

    def dot32(first, second):
        return jnp.dot(first, second, preferred_element_type=jnp.float32)

    def reflect(block_pivot, block_rest, vectors_pivot, vectors_rest):
        partial_value = jnp.einsum(
            "ik,ir->kr", vectors_pivot[1], block_pivot, preferred_element_type=jnp.float32
        )
        partial_value = partial_value + jnp.einsum(
            "ik,ir->kr", vectors_rest[1], block_rest, preferred_element_type=jnp.float32
        )
        summed = lax.psum(partial_value.astype(jnp.bfloat16), "front")
        pivots = block_pivot - dot32(vectors_pivot[0], summed)
        rest = block_rest - dot32(vectors_rest[0], summed)
        return (pivots.astype(jnp.bfloat16), rest.astype(jnp.bfloat16))

    def one_hot(rows, places):
        return rows[:, None] == places[None, :]

    pivot_rows = front_index * pivot_count + jnp.arange(pivot_count, dtype=jnp.int32)
    rest_rows = depth + front_index * rest_count + jnp.arange(rest_count, dtype=jnp.int32)
    pivot_hits = one_hot(pivot_rows, stack_place[0])
    rest_hits = one_hot(rest_rows, stack_place[0])

    def assemble(joined):
        def fill_rows(own_rows, hits):
            count = joined.shape[0]
            picked_rows = dot32(hits[:, :count].astype(jnp.bfloat16), joined)
            filled = jnp.any(hits, axis=1)[:, None]
            return jnp.where(filled, picked_rows.astype(jnp.bfloat16), own_rows)

        return (fill_rows(node_pivot_block[0], pivot_hits), fill_rows(node_rest_block[0], rest_hits))

    rest_vectors = lax.all_gather(node_vectors_rest[0, 0], "front", axis=0, tiled=True)

    def product(vectors):
        value = jnp.einsum("ck,ik->ci", rest_vectors, vectors, preferred_element_type=jnp.float32)
        return value.astype(jnp.bfloat16)

    rest_by_pivot = product(node_vectors_pivot[0, 1])
    rest_by_rest = product(node_vectors_rest[0, 1])

    def pass_rest(left_whole, right_whole):
        stack_pivots, stack_rest = assemble(jnp.concatenate([left_whole, right_whole], axis=0))
        own = lax.dynamic_update_slice(
            jnp.zeros((rest_rows_all, stack_rest.shape[1]), jnp.float32),
            stack_rest.astype(jnp.float32),
            (front_index * rest_count, 0),
        )
        partial_value = own - dot32(rest_by_pivot, stack_pivots) - dot32(rest_by_rest, stack_rest)
        return lax.psum(partial_value.astype(jnp.bfloat16), "front")

    leaf_pivots, leaf_remainder = reflect(
        leaf_pivot_block[0], leaf_rest_block[0], leaf_vectors_pivot[0], leaf_vectors_rest[0]
    )
    whole = lax.all_gather(leaf_remainder, "front", axis=0, tiled=True)
    whole = pass_rest(from_behind(whole, "leaf", 1), whole)
    for height in range(2, LEVELS + 1):
        offset = 2 ** (height - 2)
        whole = pass_rest(from_behind(whole, "leaf", offset), from_behind(whole, "leaf", -offset))
    root_whole = from_behind(whole, "leaf", -(subtree // 2))
    stack_pivots, stack_rest = assemble(root_whole)
    node_pivots, node_remainder = reflect(
        stack_pivots, stack_rest, node_vectors_pivot[0], node_vectors_rest[0]
    )
    pivots_own = (leaf_pivots, node_pivots)

    def settle(which_slot, parent_part):
        right_side = pivots_own[which_slot].astype(jnp.float32)
        if parent_part is not None:
            hits = one_hot(parent_columns[0, which_slot], pivot_rows).astype(jnp.bfloat16)
            chosen = lax.psum(dot32(hits, parent_part).astype(jnp.bfloat16), "front")
            right_side = right_side - dot32(coupling[0, which_slot], chosen)
        gathered = lax.all_gather(right_side.astype(jnp.bfloat16), "front", axis=0, tiled=True)
        return dot32(pivot_inverse[0, which_slot], gathered).astype(jnp.bfloat16)

    node_solution = settle(1, None)
    for height in range(LEVELS, 0, -1):
        if height == LEVELS:
            parent_part = from_behind(node_solution, "leaf", subtree // 2)
        else:
            offset = 2 ** (height - 1)
            lower_part = from_behind(node_solution, "leaf", offset)
            higher_part = from_behind(node_solution, "leaf", -offset)
            parent_part = added(higher_part, lower_part)
        node_solution = settle(1, parent_part)
    from_right = from_behind(node_solution, "leaf", -1)
    parent_part = added(from_right, node_solution)
    leaf_solution = settle(0, parent_part)
    solution = jnp.stack([leaf_solution, node_solution])[None]
    return (solution, node_remainder[None])


def solution(mesh):
    in_specs = (
        P("leaf", "front", None),
        P("leaf", "front", None),
        P("leaf", "front", None),
        P("leaf", "front", None),
        P("leaf", None, "front", None),
        P("leaf", None, "front", None),
        P("leaf", None, "front", None),
        P("leaf", None, "front", None),
        P("leaf", None),
        P("leaf", None, None),
        P("leaf", None, "front", None),
        P("leaf", None, "front", None),
    )
    out_specs = (P("leaf", None, "front", None), P("leaf", "front", None))
    return jax.shard_map(
        per_device, mesh=mesh, in_specs=in_specs, out_specs=out_specs, check_vma=False
    )
```
